256 devices in a mesh: rep: 4 (over y, x), section: 2 (over core), wide: 32 (over z).
Axes of the slice: x: 2, y: 2, z: 32, core: 2. Of those that a mesh axis runs over, the one named last changes fastest.
The devices are a block of a 4x8x32 slice.
Arguments:
- acts: bfloat16 [2, 1024, 8192], P('section', 'rep', 'wide'), parts along dimension 1, may hold values from -100 to 100
- norm_gain: bfloat16 [2, 8192], P('section', 'wide'), may hold values from 0.099609375 to 1.8984375
- w_qkv: bfloat16 [2, 8192, 5120], P('section', None, 'wide'), may hold values from -0.0625 to 0.0625
- w_out: bfloat16 [2, 4096, 8192], P('section', None, 'wide'), may hold values from -0.5 to 0.5
- key_cache: bfloat16 [2, 1024, 384, 512], P('section', ('rep', 'wide')), parts along dimension 1, may hold values from -400 to 400
- value_cache: bfloat16 [2, 1024, 384, 512], P('section', ('rep', 'wide')), parts along dimension 1, may hold values from -6 to 6
- cache_lengths: int32 [2, 1024], P('section', ('rep', 'wide')), parts along dimension 1, may hold values from 2 to 384, as said below
- slot_of: int32 [2, 1024], P('section', 'rep'), parts along dimension 1, may hold values from 0 to 255, each once within a row
Outputs:
- handed: bfloat16 [2, 1024, 8192], P('section', 'rep', 'wide'), parts along dimension 1
The draws below stay inside these ranges and needn't reach their ends.
There are 4 independent parts, one for each index of `rep`. The reference program is written for one: setup_inputs(seed, part) draws one part's arguments, and reference() takes and returns one part's arrays. A program takes and returns all parts, laid end to end along the dimension named above; an argument that names none is the same for every part. Nothing has to cross between parts.
Inputs may be any that keep to these rules, and one draw needn't show every extreme that they name: `cache_lengths`: slot j of a section belongs to owner j // 8; in every section some slot holds exactly 384. `slot_of`: each section's row names every slot once.
All inputs are finite; a program needn't handle non-finite values.
Results may differ from the reference program's by a relative error of at most 0.005.
Values may be sent and summed in bfloat16 or wider, within the bound.
No kernel may reach another device: no remote copies, remote signals or barrier semaphores. Data moves between devices by JAX's collectives and lax.ppermute only.
A program may use at most 64 MiB of HBM per device.

```python
import math
import jax
import jax.numpy as jnp
from jax import lax

D = 8192
HEADS = 32
KV_HEADS = 4
HDIM = 128
LMAX = 384
REQ_DEV = 8
SECTIONS = 2
REQUESTS = 256
QKV = 5120


def draw_acts(key, part):
    streams = jax.random.split(key, 4)
    values_raw = jax.random.normal(streams[0], (SECTIONS, REQUESTS, D), jnp.float32)
    column = jnp.arange(D, dtype=jnp.float32) / max(D - 1, 1)
    jitter = jnp.exp(jax.random.uniform(streams[3], (SECTIONS, 1, D), jnp.float32, -0.6, 0.6))
    column_rise = jnp.exp(math.log(3.0) * column)
    row_scale = jnp.exp(jax.random.uniform(streams[1], (SECTIONS, REQUESTS, 1), jnp.float32, math.log(0.3), math.log(3.0)))
    return jnp.clip(values_raw * row_scale * column_rise * jitter, -100.0, 100.0).astype(jnp.bfloat16)


def draw_key_cache(key, part):
    streams = jax.random.split(key, 1)
    width_all = KV_HEADS * HDIM
    values_raw = jnp.clip(jax.random.normal(streams[0], (SECTIONS, REQUESTS, LMAX, width_all), jnp.float32), -6.0, 6.0)
    return jnp.clip(values_raw, -400.0, 400.0).astype(jnp.bfloat16)


def draw_cache_lengths(key, part):
    streams = jax.random.split(key, 3)
    owners = REQUESTS // REQ_DEV
    shifts = jax.random.randint(streams[0], (SECTIONS, owners, 1), 0, 4)
    ceiling = jnp.maximum(jnp.right_shift(jnp.int32(LMAX), shifts), 2)
    lengths_raw = 2 + jax.random.randint(streams[1], (SECTIONS, owners, REQ_DEV), 0, ceiling - 1)
    lengths_flat = lengths_raw.reshape(SECTIONS, REQUESTS)
    chosen = jax.random.randint(streams[2], (SECTIONS,), 0, REQUESTS)
    section_rows = jnp.arange(SECTIONS, dtype=jnp.int32)
    lengths_flat = lengths_flat.at[section_rows, chosen].set(LMAX)
    return lengths_flat.astype(jnp.int32)


def shard_levels(own_key, extent, pieces, smallest, top_value):
    loudness, own = 1.0, jax.random.fold_in(own_key, 6)
    for axis_at, blocks in pieces:
        draws = jnp.exp(jax.random.uniform(jax.random.fold_in(own, axis_at), (blocks,), jnp.float32, smallest / len(pieces), top_value / len(pieces)))
        loudness = loudness * jnp.repeat(draws, extent[axis_at] // blocks).reshape([-1 if axis == axis_at else 1 for axis in range(len(extent))])
    return loudness


def centred(own_key, dims, scale, reach, pieces=(), kind=jnp.bfloat16):
    result = scale * jax.random.normal(own_key, dims, jnp.float32)
    if pieces:
        result = result * shard_levels(own_key, dims, pieces, -0.22, 0.18)
    return jnp.clip(result, -reach, reach).astype(kind)


def setup_inputs(seed: int = 0, part: int = 0) -> dict:
    arg_keys = jax.random.split(jax.random.key(seed), 9)
    own_keys = jax.random.split(jax.random.fold_in(arg_keys[8], part), 9)
    acts = draw_acts(jax.random.fold_in(jax.random.fold_in(arg_keys[8], part), 71), part)
    norm_gain = jnp.clip(1.0 + 0.18 * jax.random.normal(arg_keys[1], (SECTIONS, D), jnp.float32), 0.099609375, 1.8984375).astype(jnp.bfloat16)
    w_qkv = centred(arg_keys[2], (SECTIONS, D, QKV), D ** -0.5, 0.0625, ((0, 2), (2, 32)))
    w_out = centred(arg_keys[3], (SECTIONS, HEADS * HDIM, D), HDIM ** -0.5, 0.5, ((0, 2), (2, 32)))
    key_cache = draw_key_cache(jax.random.fold_in(jax.random.fold_in(arg_keys[8], part), 71), part)
    value_cache = centred(own_keys[5], (SECTIONS, REQUESTS, LMAX, KV_HEADS * HDIM), 1.0, 6.0, ((0, 2), (1, 32)))
    cache_lengths = draw_cache_lengths(jax.random.fold_in(jax.random.fold_in(arg_keys[8], part), 71), part)
    slot_of = jax.vmap(lambda own: jax.random.permutation(own, REQUESTS))(jax.random.split(own_keys[7], SECTIONS)).reshape((SECTIONS, REQUESTS)).astype(jnp.int32)
    return {"acts": acts, "norm_gain": norm_gain, "w_qkv": w_qkv, "w_out": w_out, "key_cache": key_cache, "value_cache": value_cache, "cache_lengths": cache_lengths, "slot_of": slot_of}


epsilon = 1e-05
rope_base = 500000.0
masked_score = -1e+30

def rounded(values):
    return lax.optimization_barrier(values.astype(jnp.bfloat16)).astype(jnp.float32)

def rotate(values, position):
    half_dim = HDIM // 2
    exponent = jnp.arange(half_dim, dtype=jnp.float32) * (2.0 / HDIM)
    frequency = jnp.exp(-math.log(rope_base) * exponent)
    angle = position[..., None] * frequency
    cosine = jnp.cos(angle)
    sine = jnp.sin(angle)
    first_half = values[..., :half_dim]
    second_half = values[..., half_dim:]
    return jnp.concatenate([first_half * cosine - second_half * sine, second_half * cosine + first_half * sine], axis=-1)

def attend(joined_rows, key_rows, value_rows, lengths_here):
    row_count = joined_rows.shape[0]
    groups = HEADS // KV_HEADS
    query_width = HEADS * HDIM
    kv_width = KV_HEADS * HDIM
    queries = joined_rows[:, :query_width].reshape(row_count, KV_HEADS, groups, HDIM).astype(jnp.float32)
    new_keys = joined_rows[:, query_width:query_width + kv_width].reshape(row_count, KV_HEADS, HDIM).astype(jnp.float32)
    new_values = joined_rows[:, query_width + kv_width:].reshape(row_count, KV_HEADS, HDIM).astype(jnp.float32)
    position = lengths_here.astype(jnp.float32)
    query_wide = rounded(rotate(queries, position[:, None, None]))
    key_wide = rounded(rotate(new_keys, position[:, None]))
    score_scale = 1.0 / math.sqrt(HDIM)
    cache_span = key_rows.shape[1]
    cached_keys = key_rows.reshape(row_count, cache_span, KV_HEADS, HDIM).astype(jnp.float32)
    cached_values = value_rows.reshape(row_count, cache_span, KV_HEADS, HDIM).astype(jnp.float32)
    scores = jnp.einsum('ngqd,nlgd->ngql', query_wide, cached_keys) * score_scale
    own_score = jnp.einsum('ngqd,ngd->ngq', query_wide, key_wide) * score_scale
    live_mask = (jnp.arange(cache_span, dtype=jnp.int32)[None, :] < lengths_here[:, None])[:, None, None, :]
    masked = jnp.where(live_mask, scores, masked_score)
    peak = jnp.maximum(lax.optimization_barrier(jnp.max(masked, axis=-1)), own_score)
    weights = jnp.where(live_mask, jnp.exp(masked - peak[..., None]), 0.0)
    own_weight = jnp.exp(own_score - peak)
    denominator = lax.optimization_barrier(jnp.sum(weights, axis=-1)) + own_weight
    weighted = jnp.einsum('ngql,nlgd->ngqd', rounded(weights), cached_values)
    weighted = weighted + rounded(own_weight)[..., None] * new_values[:, :, None, :]
    return (weighted / denominator[..., None]).reshape(row_count, query_width).astype(jnp.bfloat16)

def reference(acts, norm_gain, w_qkv, w_out, key_cache, value_cache, cache_lengths, slot_of):
    results = []
    for section_index in range(SECTIONS):
        tokens = acts[section_index].astype(jnp.float32)
        squares = lax.optimization_barrier(jnp.sum(tokens * tokens, axis=1))
        normed = (tokens * lax.rsqrt(squares / D + epsilon)[:, None] * norm_gain[section_index].astype(jnp.float32)).astype(jnp.bfloat16)
        joined_rows = jnp.dot(normed, w_qkv[section_index], preferred_element_type=jnp.float32).astype(jnp.bfloat16)
        slot_table = slot_of[section_index]
        request_at_slot = jnp.zeros((REQUESTS,), jnp.int32).at[slot_table].set(jnp.arange(REQUESTS, dtype=jnp.int32))
        attended = attend(joined_rows[request_at_slot], key_cache[section_index], value_cache[section_index], cache_lengths[section_index])
        projected = jnp.dot(attended[slot_table], w_out[section_index], preferred_element_type=jnp.float32)
        results.append((tokens + projected).astype(jnp.bfloat16))
    return jnp.stack([results[-1]] + results[:-1])
```

```python
import functools
import math

import jax
import jax.numpy as jnp
from jax import lax
from jax.experimental import pallas as pl
from jax.experimental.pallas import tpu as pltpu
from jax.sharding import PartitionSpec as P


KV_HEADS = 4
HDIM = 128
EPSILON = 1e-05
ROPE_BASE = 500000.0
MASKED = -1e30


VMEM = pl.BlockSpec(memory_space=pltpu.VMEM)
SMEM = pl.BlockSpec(memory_space=pltpu.SMEM)
NT = (((1,), (1,)), ((), ()))
TN = (((0,), (0,)), ((), ()))


def shifted(value, axis, steps):
    count = lax.axis_size(axis)
    return lax.ppermute(value, axis, [(i, (i + steps) % count) for i in range(count)])


def gather_rounds(block, axis):
    count = lax.axis_size(axis)
    half = count // 2
    have = {0: block}
    rounds = []
    for at in range(0, half, 2):
        new = {}
        for hop in (2, 1):
            offset = at + hop
            if offset > half:
                continue
            new[-offset] = shifted(have[-at], axis, hop)
            if offset < half:
                new[offset] = shifted(have[at], axis, -hop)
        have.update(new)
        rounds.append(new)
    return rounds


def params(mib):
    return pltpu.CompilerParams(vmem_limit_bytes=mib << 20)


def project_kernel(axis, offsets, first, *refs):
    n = len(offsets)
    blocks, weight = refs[:n], refs[n]
    old_total, old_squares = (None, None) if first else refs[n + 1 : n + 3]
    total, squares = refs[-2:]
    count, me = lax.axis_size(axis), lax.axis_index(axis)
    requests, width = squares.shape
    gathered = None if first else old_total[...]
    summed = None if first else old_squares[...]
    for offset, ref in zip(offsets, blocks):
        values = ref[0:requests, :].astype(jnp.float32)
        gain = ref[requests : requests + 8, :][0:1].astype(jnp.float32)
        at = pl.multiple_of(lax.rem(me + (offset + count), count) * width, width)
        part = lax.dot_general(
            (values * gain).astype(jnp.bfloat16),
            weight[:, pl.ds(at, width)],
            NT,
            preferred_element_type=jnp.float32,
        )
        gathered = part if gathered is None else gathered + part
        square = values * values
        summed = square if summed is None else summed + square
    total[...] = gathered
    squares[...] = summed


def project(blocks, weight, state, axis):
    offsets = tuple(blocks)
    first = state is None
    width = next(iter(blocks.values())).shape[1]
    requests = next(iter(blocks.values())).shape[0] - 8
    features = weight.shape[0]
    return pl.pallas_call(
        functools.partial(project_kernel, axis, offsets, first),
        out_shape=(
            jax.ShapeDtypeStruct((requests, features), jnp.float32),
            jax.ShapeDtypeStruct((requests, width), jnp.float32),
        ),
        in_specs=[VMEM] * (len(offsets) + 1 + (0 if first else 2)),
        out_specs=(VMEM, VMEM),
        compiler_params=params(24),
        cost_estimate=pl.CostEstimate(
            flops=2 * requests * width * features * len(offsets), transcendentals=0, bytes_accessed=0
        ),
    )(*blocks.values(), weight, *(() if first else state))


def by_slot_kernel(model_width, total, squares, slots, out):
    scale = lax.rsqrt(jnp.sum(squares[...], axis=1, keepdims=True) / model_width + EPSILON)
    joined = (total[...] * scale).astype(jnp.bfloat16)
    requests = joined.shape[0]
    slot = lax.broadcasted_iota(jnp.int32, (requests, requests), 0)
    pick = jnp.where(slot == slots[...], 1.0, 0.0).astype(jnp.bfloat16)
    out[...] = jnp.dot(pick, joined, preferred_element_type=jnp.float32).astype(jnp.bfloat16)


def by_slot(state, slots, model_width):
    total, squares = state
    return pl.pallas_call(
        functools.partial(by_slot_kernel, model_width),
        out_shape=jax.ShapeDtypeStruct(total.shape, jnp.bfloat16),
        in_specs=[VMEM] * 3,
        out_specs=VMEM,
        compiler_params=params(24),
    )(total, squares, slots)


def attend_kernel(heads, lengths, joined, cosine, sine, keys, values, out, queries, attended):
    slots, span = keys.shape[0], keys.shape[1]
    groups = heads // KV_HEADS
    turn, cross = cosine[...], sine[...]

    def head(at):
        return joined[:, at * HDIM : (at + 1) * HDIM].astype(jnp.float32)

    def rotated(at):
        value = head(at)
        value = value * turn + pltpu.roll(value, HDIM // 2, 1) * cross
        return value.astype(jnp.bfloat16).astype(jnp.float32)

    for at in range(heads + KV_HEADS):
        queries[at] = rotated(at)
    for at in range(KV_HEADS):
        queries[heads + KV_HEADS + at] = head(heads + KV_HEADS + at)
    scale = 1.0 / math.sqrt(HDIM)
    lane_group = lax.broadcasted_iota(jnp.int32, (heads, KV_HEADS * HDIM), 1) // HDIM
    row_group = lax.broadcasted_iota(jnp.int32, (heads, KV_HEADS * HDIM), 0) // groups
    own_lanes = lane_group == row_group
    position = lax.broadcasted_iota(jnp.int32, (heads, span), 1)
    for slot in range(slots):
        rows = queries[:, slot, :]
        query = rows[0:heads]
        new_keys = rows[heads : heads + KV_HEADS]
        new_values = rows[heads + KV_HEADS :]
        key_rows = jnp.concatenate(
            [jnp.broadcast_to(new_keys[g : g + 1], (groups, HDIM)) for g in range(KV_HEADS)], 0
        )
        value_rows = jnp.concatenate(
            [jnp.broadcast_to(new_values[g : g + 1], (groups, HDIM)) for g in range(KV_HEADS)], 0
        )
        own = jnp.sum(query * key_rows, axis=1, keepdims=True) * scale
        wide = jnp.where(own_lanes, jnp.concatenate([query] * KV_HEADS, 1), 0.0).astype(jnp.bfloat16)
        scores = (
            lax.dot_general(wide, keys[slot], NT, preferred_element_type=jnp.float32) * scale
        )
        live = position < lengths[slot]
        scores = jnp.where(live, scores, MASKED)
        peak = jnp.maximum(jnp.max(scores, axis=1, keepdims=True), own)
        weights = jnp.where(live, jnp.exp(scores - peak), 0.0)
        own_weight = jnp.exp(own - peak)
        denominator = jnp.sum(weights, axis=1, keepdims=True) + own_weight
        mixed = jnp.dot(
            weights.astype(jnp.bfloat16), values[slot], preferred_element_type=jnp.float32
        )
        picked = jnp.concatenate(
            [
                mixed[g * groups : (g + 1) * groups, g * HDIM : (g + 1) * HDIM]
                for g in range(KV_HEADS)
            ],
            0,
        )
        picked = picked + own_weight.astype(jnp.bfloat16).astype(jnp.float32) * value_rows
        attended[:, slot, :] = picked / denominator
    for at in range(heads):
        out[:, at * HDIM : (at + 1) * HDIM] = attended[at].astype(jnp.bfloat16)


def attend(joined, cosine, sine, keys, values, lengths):
    slots = keys.shape[0]
    heads = joined.shape[1] // HDIM - 2 * KV_HEADS
    return pl.pallas_call(
        functools.partial(attend_kernel, heads),
        out_shape=jax.ShapeDtypeStruct((slots, heads * HDIM), jnp.bfloat16),
        in_specs=[SMEM] + [VMEM] * 5,
        out_specs=VMEM,
        scratch_shapes=[
            pltpu.VMEM((heads + 2 * KV_HEADS, slots, HDIM), jnp.float32),
            pltpu.VMEM((heads, slots, HDIM), jnp.float32),
        ],
        compiler_params=params(24),
    )(lengths, joined, cosine, sine, keys, values)


def finish_kernel(axis, offsets, *refs):
    n = len(offsets)
    blocks = refs[:n]
    weight, tokens, slots, out, rows = refs[n:]
    count, me = lax.axis_size(axis), lax.axis_index(axis)
    per = blocks[0].shape[0]
    requests = tokens.shape[0]
    for at, ref in enumerate(blocks):
        rows[at * per : (at + 1) * per, :] = ref[...]
    projected = jnp.dot(rows[...], weight[...], preferred_element_type=jnp.float32)
    place = lax.broadcasted_iota(jnp.int32, (requests, requests), 0)
    shift = (me + offsets[0] + count) * per
    slot = lax.rem(place + shift, requests)
    pick = jnp.where(slot == slots[...], 1.0, 0.0).astype(jnp.bfloat16)
    result = tokens[...].astype(jnp.float32)
    rest = projected
    for _ in range(3):
        piece = rest.astype(jnp.bfloat16)
        result = result + lax.dot_general(pick, piece, TN, preferred_element_type=jnp.float32)
        rest = rest - piece.astype(jnp.float32)
    out[...] = result.astype(jnp.bfloat16)


def finish(blocks, weight, tokens, slots, axis):
    offsets = tuple(sorted(blocks))
    return pl.pallas_call(
        functools.partial(finish_kernel, axis, offsets),
        out_shape=jax.ShapeDtypeStruct(tokens.shape, jnp.bfloat16),
        in_specs=[VMEM] * (len(offsets) + 3),
        out_specs=VMEM,
        scratch_shapes=[pltpu.VMEM((tokens.shape[0], weight.shape[0]), jnp.bfloat16)],
        compiler_params=params(24),
    )(*(blocks[offset] for offset in offsets), weight, tokens, slots)


def rope_tables(lengths):
    half = HDIM // 2
    exponent = jnp.arange(half, dtype=jnp.float32) * (2.0 / HDIM)
    frequency = jnp.exp(-math.log(ROPE_BASE) * exponent)
    angle = lengths.astype(jnp.float32)[:, None] * frequency
    cosine, sine = jnp.cos(angle), jnp.sin(angle)
    return jnp.concatenate([cosine, cosine], -1), jnp.concatenate([-sine, sine], -1)


def shards(acts, norm_gain, w_qkv, w_out, key_cache, value_cache, cache_lengths, slot_of):
    axis = "wide"
    tokens = acts[0]
    count = lax.axis_size(axis)
    model_width = count * tokens.shape[1]
    cosine, sine = rope_tables(cache_lengths[0])
    packed = jnp.concatenate([tokens, jnp.broadcast_to(norm_gain, (8, norm_gain.shape[1]))], axis=0)
    weight = jnp.swapaxes(w_qkv[0], 0, 1)
    state = None
    for index, new in enumerate(gather_rounds(packed, axis)):
        if index == 0:
            new = {0: packed, **new}
        state = project(new, weight, state, axis)
    sent = by_slot(state, slot_of, model_width)
    received = lax.all_to_all(
        sent.reshape(count, -1, sent.shape[1]), axis, 0, 0, tiled=True
    )
    joined = jnp.swapaxes(received, 0, 1).reshape(received.shape[1], -1)
    attended = attend(joined, cosine, sine, key_cache[0], value_cache[0], cache_lengths[0])
    blocks = {0: attended}
    for new in gather_rounds(attended, axis):
        blocks.update(new)
    updated = finish(blocks, w_out[0], tokens, slot_of, axis)
    return shifted(updated, "section", 1)[None]


def solution(mesh):
    placed = (
        P("section", "rep", "wide"),
        P("section", "wide"),
        P("section", None, "wide"),
        P("section", None, "wide"),
        P("section", ("rep", "wide"), None, None),
        P("section", ("rep", "wide"), None, None),
        P("section", ("rep", "wide")),
        P("section", "rep"),
    )
    return jax.shard_map(
        shards, mesh=mesh, in_specs=placed, out_specs=P("section", "rep", "wide"), check_vma=False
    )
```

```python
import functools
import math

import jax
import jax.numpy as jnp
from jax import lax
from jax.experimental import pallas as pl
from jax.experimental.pallas import tpu as pltpu
from jax.sharding import PartitionSpec as P


KV_HEADS = 4
HDIM = 128
EPSILON = 1e-05
ROPE_BASE = 500000.0
MASKED = -1e30


VMEM = pl.BlockSpec(memory_space=pltpu.VMEM)
SMEM = pl.BlockSpec(memory_space=pltpu.SMEM)
HBM = pl.BlockSpec(memory_space=pltpu.HBM)
NT = (((1,), (1,)), ((), ()))
TN = (((0,), (0,)), ((), ()))


def shifted(value, axis, steps):
    count = lax.axis_size(axis)
    return lax.ppermute(value, axis, [(i, (i + steps) % count) for i in range(count)])


def leaf_plan(half, batches):
    plan = {at: [] for at in range(0, half, 2)}
    for batch in batches:
        plan[batch[-1]].append((batch, 1))
        plan[min(batch[-1] + 2, half - 2)].append((batch, -1))
    return plan


def gather(block, axis, batches):
    half = lax.axis_size(axis) // 2
    have = {0: block}
    parts = [((0,), block)]
    plan = leaf_plan(half, batches)
    for at in range(0, half, 2):
        offset = at + 2
        have[-offset] = shifted(have[-at], axis, 2)
        parts.append(((-offset,), have[-offset]))
        if offset < half:
            have[offset] = shifted(have[at], axis, -2)
            parts.append(((offset,), have[offset]))
        for batch, way in plan[at]:
            sent = [have[-way * even] for even in batch]
            joined = jnp.concatenate(sent, axis=0) if len(sent) > 1 else sent[0]
            moved = shifted(joined, axis, way)
            parts.append((tuple(-way * (even + 1) for even in batch), moved))
    return parts


def params(mib):
    return pltpu.CompilerParams(vmem_limit_bytes=mib << 20)


def pack_kernel(tokens, gain, out, gain_row, semaphores):
    requests = tokens.shape[0]
    whole = pltpu.make_async_copy(tokens, out.at[0:requests, :], semaphores.at[0])
    row = pltpu.make_async_copy(gain, gain_row, semaphores.at[1])
    whole.start()
    row.start()
    row.wait()
    tail = out.shape[0] - requests
    out[requests:, :] = jnp.broadcast_to(gain_row[...], (tail, gain_row.shape[1]))
    whole.wait()


def pack(tokens, gain):
    requests, width = tokens.shape
    return pl.pallas_call(
        pack_kernel,
        out_shape=jax.ShapeDtypeStruct((requests + 8, width), tokens.dtype),
        in_specs=[HBM, HBM],
        out_specs=VMEM,
        scratch_shapes=[pltpu.VMEM(gain.shape, gain.dtype), pltpu.SemaphoreType.DMA((2,))],
        compiler_params=params(8),
    )(tokens, gain)


def project_kernel(axis, offsets, model_width, *refs):
    n = len(offsets)
    blocks = refs[:n]
    weight, slots, out, total = refs[n:]
    count, me = lax.axis_size(axis), lax.axis_index(axis)
    requests, _ = total.shape
    width = blocks[0].shape[1]
    rows = requests + 8

    def over_blocks(step, carry):
        for group, ref in zip(offsets, blocks):
            if len(group) == 1:
                carry = step(ref, 0, group[0], carry)
            else:
                stride = group[1] - group[0]

                def one(index, carry, ref=ref, first=group[0], stride=stride):
                    at = pl.multiple_of(index * rows, 8)
                    return step(ref, at, first + index * stride, carry)

                carry = lax.fori_loop(0, len(group), one, carry)
        return carry

    def square(ref, at, _, carry):
        values = ref[pl.ds(at, requests), :].astype(jnp.float32)
        values = values * values
        return carry + sum(values[:, i : i + 128] for i in range(0, width, 128))

    squares = over_blocks(square, jnp.zeros((requests, 128), jnp.float32))
    scale = lax.rsqrt(jnp.sum(squares, axis=1, keepdims=True) / model_width + EPSILON)
    total[...] = jnp.zeros_like(total)

    def multiply(ref, at, offset, carry):
        values = ref[pl.ds(at, requests), :].astype(jnp.float32)
        gain = ref[pl.ds(at + requests, 8), :][0:1].astype(jnp.float32)
        column = pl.multiple_of(lax.rem(me + (offset + count), count) * width, width)
        total[...] += lax.dot_general(
            (values * scale * gain).astype(jnp.bfloat16),
            weight[:, pl.ds(column, width)],
            NT,
            preferred_element_type=jnp.float32,
        )
        return carry

    over_blocks(multiply, 0)
    joined = total[...].astype(jnp.bfloat16)
    slot = lax.broadcasted_iota(jnp.int32, (requests, requests), 0)
    pick = jnp.where(slot == slots[...], 1.0, 0.0).astype(jnp.bfloat16)
    out[...] = jnp.dot(pick, joined, preferred_element_type=jnp.float32).astype(jnp.bfloat16)


def project(parts, weight, slots, axis):
    offsets = tuple(group for group, _ in parts)
    requests, features = slots.shape[1], weight.shape[0]
    return pl.pallas_call(
        functools.partial(project_kernel, axis, offsets, weight.shape[1]),
        out_shape=jax.ShapeDtypeStruct((requests, features), jnp.bfloat16),
        in_specs=[VMEM] * (len(parts) + 2),
        out_specs=VMEM,
        scratch_shapes=[pltpu.VMEM((requests, features), jnp.float32)],
        compiler_params=params(24),
    )(*(array for _, array in parts), weight, slots)


def attend_kernel(
    heads, lengths, joined, cosine, sine, keys, values_hbm, out,
    queries, attended, values, weights_all, numbers, semaphore,
):
    fetch = pltpu.make_async_copy(values_hbm, values, semaphore)
    fetch.start()
    slots, span = keys.shape[0], keys.shape[1]
    groups = heads // KV_HEADS
    turn, cross = cosine[...], sine[...]

    def head(at):
        return joined[:, at * HDIM : (at + 1) * HDIM].astype(jnp.float32)

    def rotated(at):
        value = head(at)
        value = value * turn + pltpu.roll(value, HDIM // 2, 1) * cross
        return value.astype(jnp.bfloat16).astype(jnp.float32)

    for at in range(heads + KV_HEADS):
        queries[at] = rotated(at)
    for at in range(KV_HEADS):
        queries[heads + KV_HEADS + at] = head(heads + KV_HEADS + at)
    scale = 1.0 / math.sqrt(HDIM)
    lane_group = lax.broadcasted_iota(jnp.int32, (heads, KV_HEADS * HDIM), 1) // HDIM
    row_group = lax.broadcasted_iota(jnp.int32, (heads, KV_HEADS * HDIM), 0) // groups
    own_lanes = lane_group == row_group
    position = lax.broadcasted_iota(jnp.int32, (heads, span), 1)

    def per_head(rows):
        return jnp.concatenate(
            [jnp.broadcast_to(rows[g : g + 1], (groups, HDIM)) for g in range(KV_HEADS)], 0
        )

    for slot in range(slots):
        rows = queries[:, slot, :]
        query = rows[0:heads]
        key_rows = per_head(rows[heads : heads + KV_HEADS])
        own = jnp.sum(query * key_rows, axis=1, keepdims=True) * scale
        wide = jnp.where(own_lanes, jnp.concatenate([query] * KV_HEADS, 1), 0.0).astype(jnp.bfloat16)
        scores = (
            lax.dot_general(wide, keys[slot], NT, preferred_element_type=jnp.float32) * scale
        )
        live = position < lengths[slot]
        scores = jnp.where(live, scores, MASKED)
        peak = jnp.maximum(jnp.max(scores, axis=1, keepdims=True), own)
        weights = jnp.where(live, jnp.exp(scores - peak), 0.0)
        own_weight = jnp.exp(own - peak)
        denominator = jnp.sum(weights, axis=1, keepdims=True) + own_weight
        weights_all[slot] = weights.astype(jnp.bfloat16)
        numbers[slot, 0] = jnp.broadcast_to(own_weight, (heads, HDIM))
        numbers[slot, 1] = jnp.broadcast_to(denominator, (heads, HDIM))
    fetch.wait()
    for slot in range(slots):
        value_rows = per_head(queries[heads + KV_HEADS :, slot, :])
        mixed = jnp.dot(weights_all[slot], values[slot], preferred_element_type=jnp.float32)
        picked = jnp.concatenate(
            [
                mixed[g * groups : (g + 1) * groups, g * HDIM : (g + 1) * HDIM]
                for g in range(KV_HEADS)
            ],
            0,
        )
        own_weight = numbers[slot, 0].astype(jnp.bfloat16).astype(jnp.float32)
        attended[:, slot, :] = (picked + own_weight * value_rows) / numbers[slot, 1]
    for at in range(heads):
        out[:, at * HDIM : (at + 1) * HDIM] = attended[at].astype(jnp.bfloat16)


def attend(joined, cosine, sine, keys, values, lengths):
    slots, span = keys.shape[0], keys.shape[1]
    heads = joined.shape[1] // HDIM - 2 * KV_HEADS
    return pl.pallas_call(
        functools.partial(attend_kernel, heads),
        out_shape=jax.ShapeDtypeStruct((slots, heads * HDIM), jnp.bfloat16),
        in_specs=[SMEM] + [VMEM] * 4 + [HBM],
        out_specs=VMEM,
        scratch_shapes=[
            pltpu.VMEM((heads + 2 * KV_HEADS, slots, HDIM), jnp.float32),
            pltpu.VMEM((heads, slots, HDIM), jnp.float32),
            pltpu.VMEM(values.shape, values.dtype),
            pltpu.VMEM((slots, heads, span), jnp.bfloat16),
            pltpu.VMEM((slots, 2, heads, HDIM), jnp.float32),
            pltpu.SemaphoreType.DMA(()),
        ],
        compiler_params=params(24),
    )(lengths, joined, cosine, sine, keys, values)


def finish_kernel(axis, offsets, *refs):
    n = len(offsets)
    blocks = refs[:n]
    weight, tokens, slots, out, rows = refs[n:]
    count, me = lax.axis_size(axis), lax.axis_index(axis)
    requests = tokens.shape[0]
    per = requests // count
    low = min(min(group) for group in offsets)
    for group, ref in zip(offsets, blocks):
        for index, offset in enumerate(group):
            at = (offset - low) * per
            rows[at : at + per, :] = ref[index * per : (index + 1) * per, :]
    rest = jnp.dot(rows[...], weight[...], preferred_element_type=jnp.float32)
    place = lax.broadcasted_iota(jnp.int32, (requests, requests), 0)
    slot = lax.rem(place + (me + low + count) * per, requests)
    pick = jnp.where(slot == slots[...], 1.0, 0.0).astype(jnp.bfloat16)
    result = tokens[...].astype(jnp.float32)
    picked = None
    for _ in range(3):
        piece = rest.astype(jnp.bfloat16)
        part = lax.dot_general(pick, piece, TN, preferred_element_type=jnp.float32)
        picked = part if picked is None else picked + part
        rest = rest - piece.astype(jnp.float32)
    out[...] = (result + picked).astype(jnp.bfloat16)


def finish(parts, weight, tokens, slots, axis):
    offsets = tuple(group for group, _ in parts)
    return pl.pallas_call(
        functools.partial(finish_kernel, axis, offsets),
        out_shape=jax.ShapeDtypeStruct(tokens.shape, jnp.bfloat16),
        in_specs=[VMEM] * (len(parts) + 3),
        out_specs=VMEM,
        scratch_shapes=[pltpu.VMEM((tokens.shape[0], weight.shape[0]), jnp.bfloat16)],
        compiler_params=params(24),
    )(*(array for _, array in parts), weight, tokens, slots)


def rope_tables(lengths):
    half = HDIM // 2
    exponent = jnp.arange(half, dtype=jnp.float32) * (2.0 / HDIM)
    frequency = jnp.exp(-math.log(ROPE_BASE) * exponent)
    angle = lengths.astype(jnp.float32)[:, None] * frequency
    cosine, sine = jnp.cos(angle), jnp.sin(angle)
    return jnp.concatenate([cosine, cosine], -1), jnp.concatenate([-sine, sine], -1)


def batches_of(half, ends):
    evens = [at for at in range(0, half, 2)]
    cuts = [end for end in ends if end < len(evens)] + [len(evens)]
    return tuple(tuple(evens[a:b]) for a, b in zip([0] + cuts[:-1], cuts))


def first_batches(half):
    return batches_of(half, (3, 6))


def second_batches(half):
    return batches_of(half, (3, 6))


def shards(acts, norm_gain, w_qkv, w_out, key_cache, value_cache, cache_lengths, slot_of):
    axis = "wide"
    tokens = acts[0]
    count = lax.axis_size(axis)
    cosine, sine = rope_tables(cache_lengths[0])
    packed = pack(tokens, norm_gain)
    weight = jnp.swapaxes(w_qkv[0], 0, 1)
    parts = gather(packed, axis, first_batches(count // 2))
    sent = project(parts, weight, slot_of, axis)
    received = lax.all_to_all(
        sent.reshape(count, -1, sent.shape[1]), axis, 0, 0, tiled=True
    )
    joined = jnp.swapaxes(received, 0, 1).reshape(received.shape[1], -1)
    attended = attend(joined, cosine, sine, key_cache[0], value_cache[0], cache_lengths[0])
    parts = gather(attended, axis, second_batches(count // 2))
    updated = finish(parts, w_out[0], tokens, slot_of, axis)
    return shifted(updated, "section", 1)[None]


def solution(mesh):
    placed = (
        P("section", "rep", "wide"),
        P("section", "wide"),
        P("section", None, "wide"),
        P("section", None, "wide"),
        P("section", ("rep", "wide"), None, None),
        P("section", ("rep", "wide"), None, None),
        P("section", ("rep", "wide")),
        P("section", "rep"),
    )
    return jax.shard_map(
        shards, mesh=mesh, in_specs=placed, out_specs=P("section", "rep", "wide"), check_vma=False
    )
```

```python
import functools
import math

import jax
import jax.numpy as jnp
from jax import lax
from jax.experimental import pallas as pl
from jax.experimental.pallas import tpu as pltpu
from jax.sharding import PartitionSpec as P


KV_HEADS = 4
HDIM = 128
EPSILON = 1e-05
ROPE_BASE = 500000.0
MASKED = -1e30


VMEM = pl.BlockSpec(memory_space=pltpu.VMEM)
SMEM = pl.BlockSpec(memory_space=pltpu.SMEM)
HBM = pl.BlockSpec(memory_space=pltpu.HBM)
NT = (((1,), (1,)), ((), ()))
TN = (((0,), (0,)), ((), ()))


def shifted(value, axis, steps):
    count = lax.axis_size(axis)
    return lax.ppermute(value, axis, [(i, (i + steps) % count) for i in range(count)])


def gather(block, axis):
    half = lax.axis_size(axis) // 2
    have = {0: block}
    for at in range(0, half, 2):
        new = {}
        for hop in (2, 1):
            offset = at + hop
            new[-offset] = shifted(have[-at], axis, hop)
            if offset < half:
                new[offset] = shifted(have[at], axis, -hop)
        have.update(new)
    return sorted(have.items())


def exchanged(value, axis, low):
    count = lax.axis_size(axis)
    pairs = [(i, (i + 1) % count if (i - low) % 2 == 0 else (i - 1) % count) for i in range(count)]
    return lax.ppermute(value, axis, pairs)


def gather_in_pairs(block, axis):
    half = lax.axis_size(axis) // 2
    even = lax.rem(lax.axis_index(axis), 2) == 0
    own, other = {0: block}, {}
    for at in range(0, half, 2):
        up = shifted(own[-at], axis, 2)
        if at + 2 < half:
            own[at + 2] = shifted(own[at], axis, -2)
            own[-at - 2] = up
        else:
            own[half] = up
        both = own[0] if at == 0 else jnp.concatenate([own[-at], own[at]], axis=0)
        moved = exchanged(both, axis, 0)
        if at == 0:
            other[0] = moved
        else:
            other[-at], other[at] = jnp.split(moved, 2, axis=0)
    last = half - 2
    edge = jnp.where(even, own[last], own[-last])
    other[half] = exchanged(edge, axis, 1)
    offsets = sorted(own)
    return [own[at] for at in offsets] + [other[at] for at in offsets], offsets[0]


def in_hbm(value):
    return pltpu.with_memory_space_constraint(value, pltpu.HBM)


def params(mib):
    return pltpu.CompilerParams(vmem_limit_bytes=mib << 20)


def pack_kernel(tokens, gain, out, gain_row, semaphores):
    requests = tokens.shape[0]
    whole = pltpu.make_async_copy(tokens, out.at[0:requests, :], semaphores.at[0])
    row = pltpu.make_async_copy(gain, gain_row, semaphores.at[1])
    whole.start()
    row.start()
    row.wait()
    tail = out.shape[0] - requests
    out[requests:, :] = jnp.broadcast_to(gain_row[...], (tail, gain_row.shape[1]))
    whole.wait()


def pack(tokens, gain):
    requests, width = tokens.shape
    return pl.pallas_call(
        pack_kernel,
        out_shape=jax.ShapeDtypeStruct((requests + 8, width), tokens.dtype),
        in_specs=[HBM, HBM],
        out_specs=VMEM,
        scratch_shapes=[pltpu.VMEM(gain.shape, gain.dtype), pltpu.SemaphoreType.DMA((2,))],
        compiler_params=params(8),
    )(in_hbm(tokens), in_hbm(gain))


def project_kernel(axis, offsets, *refs):
    n = len(offsets)
    blocks = refs[:n]
    weight, slots, out, normed = refs[n:]
    count, me = lax.axis_size(axis), lax.axis_index(axis)
    requests, model_width = normed.shape
    width = model_width // count
    squares = None
    for ref in blocks:
        for i in range(0, width, 128):
            values = ref[0:requests, i : i + 128].astype(jnp.float32)
            square = values * values
            squares = square if squares is None else squares + square
    scale = lax.rsqrt(jnp.sum(squares, axis=1, keepdims=True) / model_width + EPSILON)
    for offset, ref in zip(offsets, blocks):
        values = ref[0:requests, :].astype(jnp.float32)
        gain = ref[requests : requests + 8, :][0:1].astype(jnp.float32)
        column = pl.multiple_of(lax.rem(me + (offset + count), count) * width, width)
        normed[:, pl.ds(column, width)] = (values * scale * gain).astype(jnp.bfloat16)
    total = lax.dot_general(normed[...], weight[...], NT, preferred_element_type=jnp.float32)
    joined = total.astype(jnp.bfloat16)
    slot = lax.broadcasted_iota(jnp.int32, (requests, requests), 0)
    pick = jnp.where(slot == slots[...], 1.0, 0.0).astype(jnp.bfloat16)
    out[...] = jnp.dot(pick, joined, preferred_element_type=jnp.float32).astype(jnp.bfloat16)


def project(blocks, weight, slots, axis):
    offsets = tuple(offset for offset, _ in blocks)
    requests, features = slots.shape[1], weight.shape[0]
    return pl.pallas_call(
        functools.partial(project_kernel, axis, offsets),
        out_shape=jax.ShapeDtypeStruct((requests, features), jnp.bfloat16),
        in_specs=[VMEM] * (len(blocks) + 2),
        out_specs=VMEM,
        scratch_shapes=[pltpu.VMEM((requests, weight.shape[1]), jnp.bfloat16)],
        compiler_params=params(24),
    )(*(array for _, array in blocks), weight, slots)


def attend_kernel(
    heads, lengths, joined, cosine, sine, keys, values_hbm, out,
    queries, attended, values, weights_all, numbers, semaphore,
):
    fetch = pltpu.make_async_copy(values_hbm, values, semaphore)
    fetch.start()
    slots, span = keys.shape[0], keys.shape[1]
    groups = heads // KV_HEADS
    turn, cross = cosine[...], sine[...]

    def head(at):
        return joined[:, at * HDIM : (at + 1) * HDIM].astype(jnp.float32)

    def rotated(at):
        value = head(at)
        value = value * turn + pltpu.roll(value, HDIM // 2, 1) * cross
        return value.astype(jnp.bfloat16).astype(jnp.float32)

    for at in range(heads + KV_HEADS):
        queries[at] = rotated(at)
    for at in range(KV_HEADS):
        queries[heads + KV_HEADS + at] = head(heads + KV_HEADS + at)
    scale = 1.0 / math.sqrt(HDIM)
    lane_group = lax.broadcasted_iota(jnp.int32, (heads, KV_HEADS * HDIM), 1) // HDIM
    row_group = lax.broadcasted_iota(jnp.int32, (heads, KV_HEADS * HDIM), 0) // groups
    own_lanes = lane_group == row_group
    position = lax.broadcasted_iota(jnp.int32, (heads, span), 1)

    def per_head(rows):
        return jnp.concatenate(
            [jnp.broadcast_to(rows[g : g + 1], (groups, HDIM)) for g in range(KV_HEADS)], 0
        )

    for slot in range(slots):
        rows = queries[:, slot, :]
        query = rows[0:heads]
        key_rows = per_head(rows[heads : heads + KV_HEADS])
        own = jnp.sum(query * key_rows, axis=1, keepdims=True) * scale
        wide = jnp.where(own_lanes, jnp.concatenate([query] * KV_HEADS, 1), 0.0).astype(jnp.bfloat16)
        scores = (
            lax.dot_general(wide, keys[slot], NT, preferred_element_type=jnp.float32) * scale
        )
        live = position < lengths[slot]
        scores = jnp.where(live, scores, MASKED)
        peak = jnp.maximum(jnp.max(scores, axis=1, keepdims=True), own)
        weights = jnp.where(live, jnp.exp(scores - peak), 0.0)
        own_weight = jnp.exp(own - peak)
        denominator = jnp.sum(weights, axis=1, keepdims=True) + own_weight
        weights_all[slot] = weights.astype(jnp.bfloat16)
        numbers[slot, 0] = jnp.broadcast_to(own_weight, (heads, HDIM))
        numbers[slot, 1] = jnp.broadcast_to(denominator, (heads, HDIM))
    fetch.wait()
    for slot in range(slots):
        value_rows = per_head(queries[heads + KV_HEADS :, slot, :])
        mixed = jnp.dot(weights_all[slot], values[slot], preferred_element_type=jnp.float32)
        picked = jnp.concatenate(
            [
                mixed[g * groups : (g + 1) * groups, g * HDIM : (g + 1) * HDIM]
                for g in range(KV_HEADS)
            ],
            0,
        )
        own_weight = numbers[slot, 0].astype(jnp.bfloat16).astype(jnp.float32)
        attended[:, slot, :] = (picked + own_weight * value_rows) / numbers[slot, 1]
    for at in range(heads):
        out[:, at * HDIM : (at + 1) * HDIM] = attended[at].astype(jnp.bfloat16)


def attend(joined, cosine, sine, keys, values, lengths):
    slots, span = keys.shape[0], keys.shape[1]
    heads = joined.shape[1] // HDIM - 2 * KV_HEADS
    return pl.pallas_call(
        functools.partial(attend_kernel, heads),
        out_shape=jax.ShapeDtypeStruct((slots, heads * HDIM), jnp.bfloat16),
        in_specs=[SMEM] + [VMEM] * 4 + [HBM],
        out_specs=VMEM,
        scratch_shapes=[
            pltpu.VMEM((heads + 2 * KV_HEADS, slots, HDIM), jnp.float32),
            pltpu.VMEM((heads, slots, HDIM), jnp.float32),
            pltpu.VMEM(values.shape, values.dtype),
            pltpu.VMEM((slots, heads, span), jnp.bfloat16),
            pltpu.VMEM((slots, 2, heads, HDIM), jnp.float32),
            pltpu.SemaphoreType.DMA(()),
        ],
        compiler_params=params(24),
    )(lengths, joined, cosine, sine, keys, in_hbm(values))


def finish_kernel(axis, low, *refs):
    weight, tokens, slots, out, rows = refs[-5:]
    blocks = refs[:-5]
    count, me = lax.axis_size(axis), lax.axis_index(axis)
    requests = tokens.shape[0]
    per = requests // count
    for index, ref in enumerate(blocks):
        rows[index * per : (index + 1) * per, :] = ref[...]
    rest = jnp.dot(rows[...], weight[...], preferred_element_type=jnp.float32)
    partner = me + 1 - 2 * lax.rem(me, 2)
    place = lax.broadcasted_iota(jnp.int32, (requests, requests), 0)
    block = place // per
    second = block >= count // 2
    offset = low + 2 * jnp.where(second, block - count // 2, block)
    owner = lax.rem(jnp.where(second, partner, me) + offset + count, count)
    slot = owner * per + lax.rem(place, per)
    pick = jnp.where(slot == slots[...], 1.0, 0.0).astype(jnp.bfloat16)
    picked = None
    for _ in range(3):
        piece = rest.astype(jnp.bfloat16)
        part = lax.dot_general(pick, piece, TN, preferred_element_type=jnp.float32)
        picked = part if picked is None else picked + part
        rest = rest - piece.astype(jnp.float32)
    out[...] = (tokens[...].astype(jnp.float32) + picked).astype(jnp.bfloat16)


def finish(blocks, low, weight, tokens, slots, axis):
    return pl.pallas_call(
        functools.partial(finish_kernel, axis, low),
        out_shape=jax.ShapeDtypeStruct(tokens.shape, jnp.bfloat16),
        in_specs=[VMEM] * (len(blocks) + 3),
        out_specs=VMEM,
        scratch_shapes=[pltpu.VMEM((tokens.shape[0], weight.shape[0]), jnp.bfloat16)],
        compiler_params=params(24),
    )(*blocks, weight, tokens, slots)


def rope_tables(lengths):
    half = HDIM // 2
    exponent = jnp.arange(half, dtype=jnp.float32) * (2.0 / HDIM)
    frequency = jnp.exp(-math.log(ROPE_BASE) * exponent)
    angle = lengths.astype(jnp.float32)[:, None] * frequency
    cosine, sine = jnp.cos(angle), jnp.sin(angle)
    return jnp.concatenate([cosine, cosine], -1), jnp.concatenate([-sine, sine], -1)


def shards(acts, norm_gain, w_qkv, w_out, key_cache, value_cache, cache_lengths, slot_of):
    axis = "wide"
    tokens = acts[0]
    count = lax.axis_size(axis)
    cosine, sine = rope_tables(cache_lengths[0])
    packed = pack(tokens, norm_gain)
    weight = jnp.swapaxes(w_qkv[0], 0, 1)
    sent = project(gather(packed, axis), weight, slot_of, axis)
    received = lax.all_to_all(
        sent.reshape(count, -1, sent.shape[1]), axis, 0, 0, tiled=True
    )
    joined = jnp.swapaxes(received, 0, 1).reshape(received.shape[1], -1)
    attended = attend(joined, cosine, sine, key_cache[0], value_cache[0], cache_lengths[0])
    blocks, low = gather_in_pairs(attended, axis)
    updated = finish(blocks, low, w_out[0], tokens, slot_of, axis)
    return shifted(updated, "section", 1)[None]


def solution(mesh):
    placed = (
        P("section", "rep", "wide"),
        P("section", "wide"),
        P("section", None, "wide"),
        P("section", None, "wide"),
        P("section", ("rep", "wide"), None, None),
        P("section", ("rep", "wide"), None, None),
        P("section", ("rep", "wide")),
        P("section", "rep"),
    )
    return jax.shard_map(
        shards, mesh=mesh, in_specs=placed, out_specs=P("section", "rep", "wide"), check_vma=False
    )
```

```python
import functools
import math

import jax
import jax.numpy as jnp
from jax import lax
from jax.experimental import pallas as pl
from jax.experimental.pallas import tpu as pltpu
from jax.sharding import PartitionSpec as P


KV_HEADS = 4
HDIM = 128
EPSILON = 1e-05
ROPE_BASE = 500000.0
MASKED = -1e30


VMEM = pl.BlockSpec(memory_space=pltpu.VMEM)
SMEM = pl.BlockSpec(memory_space=pltpu.SMEM)
HBM = pl.BlockSpec(memory_space=pltpu.HBM)
NT = (((1,), (1,)), ((), ()))
TN = (((0,), (0,)), ((), ()))


def shifted(value, axis, steps):
    count = lax.axis_size(axis)
    return lax.ppermute(value, axis, [(i, (i + steps) % count) for i in range(count)])


def gather(block, axis):
    half = lax.axis_size(axis) // 2
    have = {0: block}
    for at in range(0, half, 2):
        new = {}
        for hop in (2, 1):
            offset = at + hop
            new[-offset] = shifted(have[-at], axis, hop)
            if offset < half:
                new[offset] = shifted(have[at], axis, -hop)
        have.update(new)
    return sorted(have.items())


def exchanged(value, axis, low):
    count = lax.axis_size(axis)
    pairs = [(i, (i + 1) % count if (i - low) % 2 == 0 else (i - 1) % count) for i in range(count)]
    return lax.ppermute(value, axis, pairs)


def gather_in_pairs(block, axis):
    half = lax.axis_size(axis) // 2
    even = lax.rem(lax.axis_index(axis), 2) == 0
    own, other = {0: block}, {}
    for at in range(0, half, 2):
        up = shifted(own[-at], axis, 2)
        if at + 2 < half:
            own[at + 2] = shifted(own[at], axis, -2)
            own[-at - 2] = up
        else:
            own[half] = up
        both = own[0] if at == 0 else jnp.concatenate([own[-at], own[at]], axis=0)
        moved = exchanged(both, axis, 0)
        if at == 0:
            other[0] = moved
        else:
            other[-at], other[at] = jnp.split(moved, 2, axis=0)
    last = half - 2
    edge = jnp.where(even, own[last], own[-last])
    other[half] = exchanged(edge, axis, 1)
    offsets = sorted(own)
    return [own[at] for at in offsets] + [other[at] for at in offsets], offsets[0]


def in_hbm(value):
    return pltpu.with_memory_space_constraint(value, pltpu.HBM)


def params(mib):
    return pltpu.CompilerParams(vmem_limit_bytes=mib << 20)


def pack_kernel(tokens, gain, out, gain_row, semaphores):
    requests = tokens.shape[0]
    whole = pltpu.make_async_copy(tokens, out.at[0:requests, :], semaphores.at[0])
    row = pltpu.make_async_copy(gain, gain_row, semaphores.at[1])
    whole.start()
    row.start()
    row.wait()
    tail = out.shape[0] - requests
    out[requests:, :] = jnp.broadcast_to(gain_row[...], (tail, gain_row.shape[1]))
    whole.wait()


def pack(tokens, gain):
    requests, width = tokens.shape
    return pl.pallas_call(
        pack_kernel,
        out_shape=jax.ShapeDtypeStruct((requests + 8, width), tokens.dtype),
        in_specs=[HBM, HBM],
        out_specs=VMEM,
        scratch_shapes=[pltpu.VMEM(gain.shape, gain.dtype), pltpu.SemaphoreType.DMA((2,))],
        compiler_params=params(8),
    )(in_hbm(tokens), in_hbm(gain))


def norm_kernel(axis, offsets, *refs):
    blocks, normed = refs[:-1], refs[-1]
    count, me = lax.axis_size(axis), lax.axis_index(axis)
    requests, model_width = normed.shape
    width = model_width // count
    squares = None
    for ref in blocks:
        for i in range(0, width, 128):
            values = ref[0:requests, i : i + 128].astype(jnp.float32)
            square = values * values
            squares = square if squares is None else squares + square
    scale = lax.rsqrt(jnp.sum(squares, axis=1, keepdims=True) / model_width + EPSILON)
    for offset, ref in zip(offsets, blocks):
        values = ref[0:requests, :].astype(jnp.float32)
        gain = ref[requests : requests + 8, :][0:1].astype(jnp.float32)
        column = pl.multiple_of(lax.rem(me + (offset + count), count) * width, width)
        normed[:, pl.ds(column, width)] = (values * scale * gain).astype(jnp.bfloat16)


def norm(blocks, requests, axis):
    offsets = tuple(offset for offset, _ in blocks)
    width = blocks[0][1].shape[1]
    return pl.pallas_call(
        functools.partial(norm_kernel, axis, offsets),
        out_shape=jax.ShapeDtypeStruct((requests, width * len(blocks)), jnp.bfloat16),
        in_specs=[VMEM] * len(blocks),
        out_specs=VMEM,
        compiler_params=params(24),
        cost_estimate=pl.CostEstimate(
            flops=40 * requests * width * len(blocks), transcendentals=0, bytes_accessed=0
        ),
    )(*(array for _, array in blocks))


def project_kernel(normed, weight, slots, out):
    requests = normed.shape[0]
    total = lax.dot_general(normed[...], weight[...], NT, preferred_element_type=jnp.float32)
    joined = total.astype(jnp.bfloat16)
    slot = lax.broadcasted_iota(jnp.int32, (requests, requests), 0)
    pick = jnp.where(slot == slots[...], 1.0, 0.0).astype(jnp.bfloat16)
    out[...] = jnp.dot(pick, joined, preferred_element_type=jnp.float32).astype(jnp.bfloat16)


def project(normed, weight, slots):
    return pl.pallas_call(
        project_kernel,
        out_shape=jax.ShapeDtypeStruct((normed.shape[0], weight.shape[0]), jnp.bfloat16),
        in_specs=[VMEM] * 3,
        out_specs=VMEM,
        compiler_params=params(24),
    )(normed, weight, slots)


def attend_kernel(
    heads, lengths, joined, cosine, sine, keys, values_hbm, out,
    queries, attended, values, weights_all, numbers, semaphore,
):
    fetch = pltpu.make_async_copy(values_hbm, values, semaphore)
    fetch.start()
    slots, span = keys.shape[0], keys.shape[1]
    groups = heads // KV_HEADS
    turn, cross = cosine[...], sine[...]

    def head(at):
        return joined[:, at * HDIM : (at + 1) * HDIM].astype(jnp.float32)

    def rotated(at):
        value = head(at)
        value = value * turn + pltpu.roll(value, HDIM // 2, 1) * cross
        return value.astype(jnp.bfloat16).astype(jnp.float32)

    for at in range(heads + KV_HEADS):
        queries[at] = rotated(at)
    for at in range(KV_HEADS):
        queries[heads + KV_HEADS + at] = head(heads + KV_HEADS + at)
    scale = 1.0 / math.sqrt(HDIM)
    lane_group = lax.broadcasted_iota(jnp.int32, (heads, KV_HEADS * HDIM), 1) // HDIM
    row_group = lax.broadcasted_iota(jnp.int32, (heads, KV_HEADS * HDIM), 0) // groups
    own_lanes = lane_group == row_group
    position = lax.broadcasted_iota(jnp.int32, (heads, span), 1)

    def per_head(rows):
        return jnp.concatenate(
            [jnp.broadcast_to(rows[g : g + 1], (groups, HDIM)) for g in range(KV_HEADS)], 0
        )

    for slot in range(slots):
        rows = queries[:, slot, :]
        query = rows[0:heads]
        key_rows = per_head(rows[heads : heads + KV_HEADS])
        own = jnp.sum(query * key_rows, axis=1, keepdims=True) * scale
        wide = jnp.where(own_lanes, jnp.concatenate([query] * KV_HEADS, 1), 0.0).astype(jnp.bfloat16)
        scores = (
            lax.dot_general(wide, keys[slot], NT, preferred_element_type=jnp.float32) * scale
        )
        live = position < lengths[slot]
        scores = jnp.where(live, scores, MASKED)
        peak = jnp.maximum(jnp.max(scores, axis=1, keepdims=True), own)
        weights = jnp.where(live, jnp.exp(scores - peak), 0.0)
        own_weight = jnp.exp(own - peak)
        denominator = jnp.sum(weights, axis=1, keepdims=True) + own_weight
        weights_all[slot] = weights.astype(jnp.bfloat16)
        numbers[slot, 0] = jnp.broadcast_to(own_weight, (heads, HDIM))
        numbers[slot, 1] = jnp.broadcast_to(denominator, (heads, HDIM))
    fetch.wait()
    for slot in range(slots):
        value_rows = per_head(queries[heads + KV_HEADS :, slot, :])
        mixed = jnp.dot(weights_all[slot], values[slot], preferred_element_type=jnp.float32)
        picked = jnp.concatenate(
            [
                mixed[g * groups : (g + 1) * groups, g * HDIM : (g + 1) * HDIM]
                for g in range(KV_HEADS)
            ],
            0,
        )
        own_weight = numbers[slot, 0].astype(jnp.bfloat16).astype(jnp.float32)
        attended[:, slot, :] = (picked + own_weight * value_rows) / numbers[slot, 1]
    for at in range(heads):
        out[:, at * HDIM : (at + 1) * HDIM] = attended[at].astype(jnp.bfloat16)


def attend(joined, cosine, sine, keys, values, lengths):
    slots, span = keys.shape[0], keys.shape[1]
    heads = joined.shape[1] // HDIM - 2 * KV_HEADS
    return pl.pallas_call(
        functools.partial(attend_kernel, heads),
        out_shape=jax.ShapeDtypeStruct((slots, heads * HDIM), jnp.bfloat16),
        in_specs=[SMEM] + [VMEM] * 4 + [HBM],
        out_specs=VMEM,
        scratch_shapes=[
            pltpu.VMEM((heads + 2 * KV_HEADS, slots, HDIM), jnp.float32),
            pltpu.VMEM((heads, slots, HDIM), jnp.float32),
            pltpu.VMEM(values.shape, values.dtype),
            pltpu.VMEM((slots, heads, span), jnp.bfloat16),
            pltpu.VMEM((slots, 2, heads, HDIM), jnp.float32),
            pltpu.SemaphoreType.DMA(()),
        ],
        compiler_params=params(24),
    )(lengths, joined, cosine, sine, keys, in_hbm(values))


def finish_kernel(axis, low, *refs):
    weight, tokens, slots, out, rows = refs[-5:]
    blocks = refs[:-5]
    count, me = lax.axis_size(axis), lax.axis_index(axis)
    requests = tokens.shape[0]
    per = requests // count
    for index, ref in enumerate(blocks):
        rows[index * per : (index + 1) * per, :] = ref[...]
    rest = jnp.dot(rows[...], weight[...], preferred_element_type=jnp.float32)
    partner = me + 1 - 2 * lax.rem(me, 2)
    place = lax.broadcasted_iota(jnp.int32, (requests, requests), 0)
    block = place // per
    second = block >= count // 2
    offset = low + 2 * jnp.where(second, block - count // 2, block)
    owner = lax.rem(jnp.where(second, partner, me) + offset + count, count)
    slot = owner * per + lax.rem(place, per)
    pick = jnp.where(slot == slots[...], 1.0, 0.0).astype(jnp.bfloat16)
    picked = None
    for _ in range(3):
        piece = rest.astype(jnp.bfloat16)
        part = lax.dot_general(pick, piece, TN, preferred_element_type=jnp.float32)
        picked = part if picked is None else picked + part
        rest = rest - piece.astype(jnp.float32)
    out[...] = (tokens[...].astype(jnp.float32) + picked).astype(jnp.bfloat16)


def finish(blocks, low, weight, tokens, slots, axis):
    return pl.pallas_call(
        functools.partial(finish_kernel, axis, low),
        out_shape=jax.ShapeDtypeStruct(tokens.shape, jnp.bfloat16),
        in_specs=[VMEM] * (len(blocks) + 3),
        out_specs=VMEM,
        scratch_shapes=[pltpu.VMEM((tokens.shape[0], weight.shape[0]), jnp.bfloat16)],
        compiler_params=params(24),
    )(*blocks, weight, tokens, slots)


def rope_tables(lengths):
    half = HDIM // 2
    exponent = jnp.arange(half, dtype=jnp.float32) * (2.0 / HDIM)
    frequency = jnp.exp(-math.log(ROPE_BASE) * exponent)
    angle = lengths.astype(jnp.float32)[:, None] * frequency
    cosine, sine = jnp.cos(angle), jnp.sin(angle)
    return jnp.concatenate([cosine, cosine], -1), jnp.concatenate([-sine, sine], -1)


def shards(acts, norm_gain, w_qkv, w_out, key_cache, value_cache, cache_lengths, slot_of):
    axis = "wide"
    tokens = acts[0]
    count = lax.axis_size(axis)
    cosine, sine = rope_tables(cache_lengths[0])
    packed = pack(tokens, norm_gain)
    weight = jnp.swapaxes(w_qkv[0], 0, 1)
    normed = norm(gather(packed, axis), tokens.shape[0], axis)
    sent = project(normed, weight, slot_of)
    received = lax.all_to_all(
        sent.reshape(count, -1, sent.shape[1]), axis, 0, 0, tiled=True
    )
    joined = jnp.swapaxes(received, 0, 1).reshape(received.shape[1], -1)
    attended = attend(joined, cosine, sine, key_cache[0], value_cache[0], cache_lengths[0])
    blocks, low = gather_in_pairs(attended, axis)
    updated = finish(blocks, low, w_out[0], tokens, slot_of, axis)
    return shifted(updated, "section", 1)[None]


def solution(mesh):
    placed = (
        P("section", "rep", "wide"),
        P("section", "wide"),
        P("section", None, "wide"),
        P("section", None, "wide"),
        P("section", ("rep", "wide"), None, None),
        P("section", ("rep", "wide"), None, None),
        P("section", ("rep", "wide")),
        P("section", "rep"),
    )
    return jax.shard_map(
        shards, mesh=mesh, in_specs=placed, out_specs=P("section", "rep", "wide"), check_vma=False
    )
```

```python
import functools
import math

import jax
import jax.numpy as jnp
from jax import lax
from jax.experimental import pallas as pl
from jax.experimental.pallas import tpu as pltpu
from jax.sharding import PartitionSpec as P


KV_HEADS = 4
HDIM = 128
CHUNK = 32
EPSILON = 1e-05
ROPE_BASE = 500000.0
MASKED = -1e30


VMEM = pl.BlockSpec(memory_space=pltpu.VMEM)
SMEM = pl.BlockSpec(memory_space=pltpu.SMEM)
HBM = pl.BlockSpec(memory_space=pltpu.HBM)
NT = (((1,), (1,)), ((), ()))
TN = (((0,), (0,)), ((), ()))


def shifted(value, axis, steps):
    count = lax.axis_size(axis)
    return lax.ppermute(value, axis, [(i, (i + steps) % count) for i in range(count)])


def gather(block, axis):
    half = lax.axis_size(axis) // 2
    have = {0: block}
    for at in range(0, half, 2):
        new = {}
        for hop in (2, 1):
            offset = at + hop
            new[-offset] = shifted(have[-at], axis, hop)
            if offset < half:
                new[offset] = shifted(have[at], axis, -hop)
        have.update(new)
    return sorted(have.items())


def exchanged(value, axis, low):
    count = lax.axis_size(axis)
    pairs = [(i, (i + 1) % count if (i - low) % 2 == 0 else (i - 1) % count) for i in range(count)]
    return lax.ppermute(value, axis, pairs)


def gather_in_pairs(block, axis):
    half = lax.axis_size(axis) // 2
    even = lax.rem(lax.axis_index(axis), 2) == 0
    own, other = {0: block}, {}
    for at in range(0, half, 2):
        up = shifted(own[-at], axis, 2)
        if at + 2 < half:
            own[at + 2] = shifted(own[at], axis, -2)
            own[-at - 2] = up
        else:
            own[half] = up
        both = own[0] if at == 0 else jnp.concatenate([own[-at], own[at]], axis=0)
        moved = exchanged(both, axis, 0)
        if at == 0:
            other[0] = moved
        else:
            other[-at], other[at] = jnp.split(moved, 2, axis=0)
    last = half - 2
    edge = jnp.where(even, own[last], own[-last])
    other[half] = exchanged(edge, axis, 1)
    offsets = sorted(own)
    return [own[at] for at in offsets] + [other[at] for at in offsets], offsets[0]


def in_hbm(value):
    return pltpu.with_memory_space_constraint(value, pltpu.HBM)


def params(mib):
    return pltpu.CompilerParams(vmem_limit_bytes=mib << 20)


def pack_kernel(tokens, gain, out, gain_row, semaphores):
    requests = tokens.shape[0]
    whole = pltpu.make_async_copy(tokens, out.at[0:requests, :], semaphores.at[0])
    row = pltpu.make_async_copy(gain, gain_row, semaphores.at[1])
    whole.start()
    row.start()
    row.wait()
    tail = out.shape[0] - requests
    out[requests:, :] = jnp.broadcast_to(gain_row[...], (tail, gain_row.shape[1]))
    whole.wait()


def pack(tokens, gain):
    requests, width = tokens.shape
    return pl.pallas_call(
        pack_kernel,
        out_shape=jax.ShapeDtypeStruct((requests + 8, width), tokens.dtype),
        in_specs=[HBM, HBM],
        out_specs=VMEM,
        scratch_shapes=[pltpu.VMEM(gain.shape, gain.dtype), pltpu.SemaphoreType.DMA((2,))],
        compiler_params=params(8),
    )(in_hbm(tokens), in_hbm(gain))


def norm_kernel(axis, offsets, *refs):
    blocks, normed = refs[:-1], refs[-1]
    count, me = lax.axis_size(axis), lax.axis_index(axis)
    requests, model_width = normed.shape
    width = model_width // count
    squares = None
    for ref in blocks:
        for i in range(0, width, 128):
            values = ref[0:requests, i : i + 128].astype(jnp.float32)
            square = values * values
            squares = square if squares is None else squares + square
    scale = lax.rsqrt(jnp.sum(squares, axis=1, keepdims=True) / model_width + EPSILON)
    for offset, ref in zip(offsets, blocks):
        values = ref[0:requests, :].astype(jnp.float32)
        gain = ref[requests : requests + 8, :][0:1].astype(jnp.float32)
        column = pl.multiple_of(lax.rem(me + (offset + count), count) * width, width)
        normed[:, pl.ds(column, width)] = (values * scale * gain).astype(jnp.bfloat16)


def norm(blocks, requests, axis):
    offsets = tuple(offset for offset, _ in blocks)
    width = blocks[0][1].shape[1]
    return pl.pallas_call(
        functools.partial(norm_kernel, axis, offsets),
        out_shape=jax.ShapeDtypeStruct((requests, width * len(blocks)), jnp.bfloat16),
        in_specs=[VMEM] * len(blocks),
        out_specs=VMEM,
        compiler_params=params(24),
        cost_estimate=pl.CostEstimate(
            flops=40 * requests * width * len(blocks), transcendentals=0, bytes_accessed=0
        ),
    )(*(array for _, array in blocks))


def project_kernel(normed, weight, slots, out):
    requests = normed.shape[0]
    total = lax.dot_general(normed[...], weight[...], NT, preferred_element_type=jnp.float32)
    joined = total.astype(jnp.bfloat16)
    across = HDIM // CHUNK
    rows = requests // across
    place = lax.broadcasted_iota(jnp.int32, (requests, requests), 0)
    slot = lax.rem(place, rows) * across + place // rows
    pick = jnp.where(slot == slots[...], 1.0, 0.0).astype(jnp.bfloat16)
    ordered = jnp.dot(pick, joined, preferred_element_type=jnp.float32)
    for piece in range(out.shape[0]):
        out[piece] = jnp.concatenate(
            [
                ordered[at * rows : (at + 1) * rows, piece * CHUNK : (piece + 1) * CHUNK]
                for at in range(across)
            ],
            axis=1,
        ).astype(jnp.bfloat16)


def project(normed, weight, slots):
    pieces, rows = weight.shape[0] // CHUNK, slots.shape[1] * CHUNK // HDIM
    return pl.pallas_call(
        project_kernel,
        out_shape=jax.ShapeDtypeStruct((pieces, rows, HDIM), jnp.bfloat16),
        in_specs=[VMEM] * 3,
        out_specs=VMEM,
        compiler_params=params(24),
    )(normed, weight, slots)


def to_owners(sent, axis):
    count = lax.axis_size(axis)
    pieces, rows, lanes = sent.shape
    by_owner = jnp.swapaxes(sent.reshape(pieces, count, rows // count, lanes), 0, 1)
    received = lax.all_to_all(by_owner, axis, 0, 0, tiled=True)
    return jnp.swapaxes(received.reshape(count * pieces, rows // count, lanes), 0, 1)


def attend_kernel(
    heads, lengths, joined, cosine, sine, keys, values_hbm, out,
    queries, attended, values, weights_all, numbers, semaphore,
):
    fetch = pltpu.make_async_copy(values_hbm, values, semaphore)
    fetch.start()
    slots, span = keys.shape[0], keys.shape[1]
    groups = heads // KV_HEADS
    turn, cross = cosine[...], sine[...]

    across = HDIM // CHUNK
    total_heads = heads + 2 * KV_HEADS
    shape = (across * total_heads, across * total_heads)
    place = lax.broadcasted_iota(jnp.int32, shape, 0)
    piece = lax.rem(place, total_heads) * across + place // total_heads
    pick = jnp.where(lax.broadcasted_iota(jnp.int32, shape, 1) == piece, 1.0, 0.0)
    pick = pick.astype(jnp.bfloat16)
    for row in range(slots // across):
        apart = jnp.dot(pick, joined[row], preferred_element_type=jnp.float32)
        for lane in range(across):
            slot = row * across + lane
            value = jnp.concatenate(
                [
                    apart[
                        at * total_heads : (at + 1) * total_heads,
                        lane * CHUNK : (lane + 1) * CHUNK,
                    ]
                    for at in range(across)
                ],
                axis=1,
            )
            turned = value * turn[slot : slot + 1] + pltpu.roll(value, HDIM // 2, 1) * (
                cross[slot : slot + 1]
            )
            queries[slot] = turned.astype(jnp.bfloat16).astype(jnp.float32)
            queries[slot, heads + KV_HEADS :, :] = value[heads + KV_HEADS :]
    scale = 1.0 / math.sqrt(HDIM)
    lane_group = lax.broadcasted_iota(jnp.int32, (heads, KV_HEADS * HDIM), 1) // HDIM
    row_group = lax.broadcasted_iota(jnp.int32, (heads, KV_HEADS * HDIM), 0) // groups
    own_lanes = lane_group == row_group
    position = lax.broadcasted_iota(jnp.int32, (heads, span), 1)

    def per_head(rows):
        return jnp.concatenate(
            [jnp.broadcast_to(rows[g : g + 1], (groups, HDIM)) for g in range(KV_HEADS)], 0
        )

    for slot in range(slots):
        rows = queries[slot]
        query = rows[0:heads]
        key_rows = per_head(rows[heads : heads + KV_HEADS])
        own = jnp.sum(query * key_rows, axis=1, keepdims=True) * scale
        wide = jnp.where(own_lanes, jnp.concatenate([query] * KV_HEADS, 1), 0.0).astype(jnp.bfloat16)
        scores = (
            lax.dot_general(wide, keys[slot], NT, preferred_element_type=jnp.float32) * scale
        )
        live = position < lengths[slot]
        scores = jnp.where(live, scores, MASKED)
        peak = jnp.maximum(jnp.max(scores, axis=1, keepdims=True), own)
        weights = jnp.where(live, jnp.exp(scores - peak), 0.0)
        own_weight = jnp.exp(own - peak)
        denominator = jnp.sum(weights, axis=1, keepdims=True) + own_weight
        weights_all[slot] = weights.astype(jnp.bfloat16)
        numbers[slot, 0] = jnp.broadcast_to(own_weight, (heads, HDIM))
        numbers[slot, 1] = jnp.broadcast_to(denominator, (heads, HDIM))
    fetch.wait()
    for slot in range(slots):
        value_rows = per_head(queries[slot, heads + KV_HEADS :, :])
        mixed = jnp.dot(weights_all[slot], values[slot], preferred_element_type=jnp.float32)
        picked = jnp.concatenate(
            [
                mixed[g * groups : (g + 1) * groups, g * HDIM : (g + 1) * HDIM]
                for g in range(KV_HEADS)
            ],
            0,
        )
        own_weight = numbers[slot, 0].astype(jnp.bfloat16).astype(jnp.float32)
        attended[:, slot, :] = (picked + own_weight * value_rows) / numbers[slot, 1]
    for at in range(heads):
        out[:, at * HDIM : (at + 1) * HDIM] = attended[at].astype(jnp.bfloat16)


def attend(joined, cosine, sine, keys, values, lengths):
    slots, span = keys.shape[0], keys.shape[1]
    heads = joined.shape[1] * CHUNK // HDIM - 2 * KV_HEADS
    return pl.pallas_call(
        functools.partial(attend_kernel, heads),
        out_shape=jax.ShapeDtypeStruct((slots, heads * HDIM), jnp.bfloat16),
        in_specs=[SMEM] + [VMEM] * 4 + [HBM],
        out_specs=VMEM,
        scratch_shapes=[
            pltpu.VMEM((slots, heads + 2 * KV_HEADS, HDIM), jnp.float32),
            pltpu.VMEM((heads, slots, HDIM), jnp.float32),
            pltpu.VMEM(values.shape, values.dtype),
            pltpu.VMEM((slots, heads, span), jnp.bfloat16),
            pltpu.VMEM((slots, 2, heads, HDIM), jnp.float32),
            pltpu.SemaphoreType.DMA(()),
        ],
        compiler_params=params(24),
    )(lengths, joined, cosine, sine, keys, in_hbm(values))


def finish_kernel(axis, low, *refs):
    weight, tokens, slots, out, rows = refs[-5:]
    blocks = refs[:-5]
    count, me = lax.axis_size(axis), lax.axis_index(axis)
    requests = tokens.shape[0]
    per = requests // count
    for index, ref in enumerate(blocks):
        rows[index * per : (index + 1) * per, :] = ref[...]
    rest = jnp.dot(rows[...], weight[...], preferred_element_type=jnp.float32)
    partner = me + 1 - 2 * lax.rem(me, 2)
    place = lax.broadcasted_iota(jnp.int32, (requests, requests), 0)
    block = place // per
    second = block >= count // 2
    offset = low + 2 * jnp.where(second, block - count // 2, block)
    owner = lax.rem(jnp.where(second, partner, me) + offset + count, count)
    slot = owner * per + lax.rem(place, per)
    pick = jnp.where(slot == slots[...], 1.0, 0.0).astype(jnp.bfloat16)
    picked = None
    for _ in range(3):
        piece = rest.astype(jnp.bfloat16)
        part = lax.dot_general(pick, piece, TN, preferred_element_type=jnp.float32)
        picked = part if picked is None else picked + part
        rest = rest - piece.astype(jnp.float32)
    out[...] = (tokens[...].astype(jnp.float32) + picked).astype(jnp.bfloat16)


def finish(blocks, low, weight, tokens, slots, axis):
    return pl.pallas_call(
        functools.partial(finish_kernel, axis, low),
        out_shape=jax.ShapeDtypeStruct(tokens.shape, jnp.bfloat16),
        in_specs=[VMEM] * (len(blocks) + 3),
        out_specs=VMEM,
        scratch_shapes=[pltpu.VMEM((tokens.shape[0], weight.shape[0]), jnp.bfloat16)],
        compiler_params=params(24),
    )(*blocks, weight, tokens, slots)


def rope_tables(lengths):
    half = HDIM // 2
    exponent = jnp.arange(half, dtype=jnp.float32) * (2.0 / HDIM)
    frequency = jnp.exp(-math.log(ROPE_BASE) * exponent)
    angle = lengths.astype(jnp.float32)[:, None] * frequency
    cosine, sine = jnp.cos(angle), jnp.sin(angle)
    return jnp.concatenate([cosine, cosine], -1), jnp.concatenate([-sine, sine], -1)


def shards(acts, norm_gain, w_qkv, w_out, key_cache, value_cache, cache_lengths, slot_of):
    axis = "wide"
    tokens = acts[0]
    cosine, sine = rope_tables(cache_lengths[0])
    packed = pack(tokens, norm_gain)
    weight = jnp.swapaxes(w_qkv[0], 0, 1)
    normed = norm(gather(packed, axis), tokens.shape[0], axis)
    sent = project(normed, weight, slot_of)
    joined = to_owners(sent, axis)
    attended = attend(joined, cosine, sine, key_cache[0], value_cache[0], cache_lengths[0])
    blocks, low = gather_in_pairs(attended, axis)
    updated = finish(blocks, low, w_out[0], tokens, slot_of, axis)
    return shifted(updated, "section", 1)[None]


def solution(mesh):
    placed = (
        P("section", "rep", "wide"),
        P("section", "wide"),
        P("section", None, "wide"),
        P("section", None, "wide"),
        P("section", ("rep", "wide"), None, None),
        P("section", ("rep", "wide"), None, None),
        P("section", ("rep", "wide")),
        P("section", "rep"),
    )
    return jax.shard_map(
        shards, mesh=mesh, in_specs=placed, out_specs=P("section", "rep", "wide"), check_vma=False
    )
```
